256 devices in a mesh: grp: 32 (over y, x, core), blk: 8 (over z).
Axes of the slice: x: 4, y: 4, z: 8, core: 2. Of those that a mesh axis runs over, the one named last changes fastest.
Arguments:
- gradient: bfloat16 [4096, 16384], P(('grp', 'blk')), may hold values from -6 to 6
- stats_left: float32 [256, 512, 512], P(('grp', 'blk')), as said below
- stats_right: float32 [256, 512, 512], P(('grp', 'blk')), as said below
- root_left: bfloat16 [256, 512, 512], P(('grp', 'blk')), may hold values from -0.25 to 0.25
- root_right: bfloat16 [256, 512, 512], P(('grp', 'blk')), may hold values from -0.25 to 0.25
- slot_block: int32 [32, 8], replicated, may hold values from 0 to 7, each once within a row
- refresh_slots: int32 [16], replicated, may hold values from 0 to 255, as said below
- newton_steps: int32 [16], replicated, may hold values from 1 to 3, as said below
Outputs:
- new_left: float32 [256, 512, 512], P(('grp', 'blk'))
- new_right: float32 [256, 512, 512], P(('grp', 'blk'))
- new_root_left: bfloat16 [256, 512, 512], P(('grp', 'blk'))
- new_root_right: bfloat16 [256, 512, 512], P(('grp', 'blk'))
- update: bfloat16 [4096, 16384], P(('grp', 'blk'))
The draws below stay inside these ranges and needn't reach their ends.
Inputs may be any that keep to these rules, and one draw needn't show every extreme that they name: `stats_left`: each matrix is symmetric positive definite. `stats_right`: each matrix is symmetric positive definite. `slot_block`: row c lists each block row once. `refresh_slots`: distinct slot numbers. `newton_steps`: not all elements are equal.
All inputs are finite; a program needn't handle non-finite values.
Results may differ from the reference program's by a relative error of at most 0.0051.
Values may be sent and summed in bfloat16 or wider, within the bound.
No kernel may reach another device: no remote copies, remote signals or barrier semaphores. Data moves between devices by JAX's collectives and lax.ppermute only.
A program may use at most 64 MiB of HBM per device.

```python
import jax
import jax.numpy as jnp
from jax import lax

B = 512
NEWTON = 3
ROWS = 4096
COLS = 16384
NBLOCKS = 256
NREF = 16
N_GRP = 32
N_BLK = 8


def definite_blocks(key):
    full_shape = (NBLOCKS, B, B)
    spread_key, noise_key = jax.random.split(key, 2)
    log_scale = jax.random.uniform(spread_key, (NBLOCKS, B), minval=jnp.log(0.1), maxval=jnp.log(2.0))
    diagonal = jnp.exp(log_scale)
    noise_field = jax.random.uniform(noise_key, full_shape, minval=-1.0, maxval=1.0)
    upper_part = jnp.triu(noise_field, 1)
    coupling_limit = 0.8 / B
    unit_matrix = coupling_limit * (upper_part + jnp.swapaxes(upper_part, 1, 2)) + jnp.eye(B, dtype=jnp.float32)
    square_root = jnp.sqrt(diagonal)
    return (square_root[:, :, None] * unit_matrix * square_root[:, None, :]).astype(jnp.float32)


def draw_stats_left(key, part):
    return definite_blocks(jax.random.fold_in(key, 17))


def draw_stats_right(key, part):
    return definite_blocks(jax.random.fold_in(key, 29))


def draw_refresh_slots(key, part):
    base_key = jax.random.fold_in(key, 43)
    pick_key, order_key = jax.random.split(base_key, 2)
    middle = 1 + jax.random.permutation(pick_key, NBLOCKS - 2)[:NREF - 2]
    ends = jnp.array([0, NBLOCKS - 1], dtype=jnp.int32)
    chosen = jnp.concatenate([ends, middle.astype(jnp.int32)])
    return jax.random.permutation(order_key, chosen).astype(jnp.int32)


def draw_newton_steps(key, part):
    base_key = jax.random.fold_in(key, 59)
    values_key, order_key = jax.random.split(base_key, 2)
    values = jax.random.randint(values_key, (NREF,), 1, NEWTON + 1, dtype=jnp.int32)
    values = values.at[0].set(1).at[1].set(NEWTON)
    return jax.random.permutation(order_key, values).astype(jnp.int32)


def level_of(rng, shape, cuts, smallest, top_value):
    factor_of = 1.0
    for position, shards_of in cuts:
        steps = jax.random.uniform(jax.random.fold_in(jax.random.fold_in(rng, 6), position), (shards_of,), jnp.float32, smallest / len(cuts), top_value / len(cuts))
        factor_of = factor_of * jnp.repeat(jnp.exp(steps), shape[position] // shards_of).reshape((-1,) + (1,) * (len(shape) - 1 - position))
    return factor_of


def gaussian(key, extent, deviation, reach, shards=(), held_as=jnp.bfloat16):
    values = deviation * jax.random.normal(key, extent, jnp.float32)
    if shards:
        values = values * level_of(key, extent, shards, -0.22, 0.18)
    return jnp.clip(values, -reach, reach).astype(held_as)


def setup_inputs(seed: int = 0) -> dict:
    key_of = jax.random.split(jax.random.key(seed), 9)
    return {
        "gradient": gaussian(key_of[0], (ROWS, COLS), 1.0, 6.0, ((0, 256),)),
        "stats_left": draw_stats_left(jax.random.fold_in(key_of[8], 71), 0),
        "stats_right": draw_stats_right(jax.random.fold_in(key_of[8], 71), 0),
        "root_left": gaussian(key_of[3], (NBLOCKS, B, B), B ** -0.5, 0.25, ((0, 256),)),
        "root_right": gaussian(key_of[4], (NBLOCKS, B, B), B ** -0.5, 0.25, ((0, 256),)),
        "slot_block": jax.vmap(lambda own: jax.random.permutation(own, N_BLK))(jax.random.split(key_of[5], N_GRP)).reshape((N_GRP, N_BLK)).astype(jnp.int32),
        "refresh_slots": draw_refresh_slots(jax.random.fold_in(key_of[8], 71), 0),
        "newton_steps": draw_newton_steps(jax.random.fold_in(key_of[8], 71), 0),
    }


damping = 0.0001
decay_rate = 0.9
root_order = 4.0

def product(left, right):
    return jnp.dot(left, right, precision=lax.Precision.HIGHEST, preferred_element_type=jnp.float32)

def inverse_root(statistic, step_count):
    identity_matrix = jnp.eye(B, dtype=jnp.float32)
    shifted = statistic + damping * identity_matrix
    frobenius = jnp.sqrt(jnp.sum(shifted * shifted))
    scaling = (1.0 + root_order) / (2.0 * frobenius)
    iterate = scaling ** (1.0 / root_order) * identity_matrix
    moving = scaling * shifted

    def newton(unused, state_pair):
        iterate, moving = state_pair
        factor = ((root_order + 1.0) * identity_matrix - moving) / root_order
        iterate = product(iterate, factor)
        factor_sq = product(factor, factor)
        moving = product(product(factor_sq, factor_sq), moving)
        return (iterate, moving)
    return lax.fori_loop(0, step_count, newton, (iterate, moving))[0]

def one_slot(items):
    grad_block, left_old, right_old, left_stored, right_stored, step_count = items
    gram_weight = (1.0 - decay_rate) / B
    left_new = decay_rate * left_old + gram_weight * jnp.dot(grad_block, grad_block.T, preferred_element_type=jnp.float32)
    right_new = decay_rate * right_old + gram_weight * jnp.dot(grad_block.T, grad_block, preferred_element_type=jnp.float32)
    refreshed = step_count > 0
    left_root = jnp.where(refreshed, inverse_root(left_new, step_count).astype(jnp.bfloat16), left_stored)
    right_root = jnp.where(refreshed, inverse_root(right_new, step_count).astype(jnp.bfloat16), right_stored)
    half_product = jnp.dot(grad_block, right_root, preferred_element_type=jnp.float32).astype(jnp.bfloat16)
    precon = jnp.dot(left_root, half_product, preferred_element_type=jnp.float32)
    grad_wide = grad_block.astype(jnp.float32)
    graft_ratio = jnp.sqrt(jnp.mean(grad_wide * grad_wide)) / jnp.sqrt(jnp.mean(precon * precon) + 1e-06)
    update_block = (precon * graft_ratio).astype(jnp.bfloat16)
    return (left_new, right_new, left_root, right_root, update_block)

def reference(gradient, stats_left, stats_right, root_left, root_right, slot_block, refresh_slots, newton_steps):
    blocks = gradient.reshape(N_BLK, B, N_GRP, B).transpose(2, 0, 1, 3)
    column_ids = jnp.arange(N_GRP, dtype=jnp.int32)[:, None]
    slot_grads = blocks[column_ids, slot_block.astype(jnp.int32)].reshape(NBLOCKS, B, B)
    slot_steps = jnp.zeros((NBLOCKS,), jnp.int32).at[refresh_slots].set(newton_steps)
    left_new, right_new, left_root, right_root, updates = lax.map(one_slot, (slot_grads, stats_left, stats_right, root_left, root_right, slot_steps))
    placed = jnp.zeros((N_GRP, N_BLK, B, B), jnp.bfloat16)
    placed = placed.at[column_ids, slot_block.astype(jnp.int32)].set(updates.reshape(N_GRP, N_BLK, B, B))
    update = placed.transpose(1, 2, 0, 3).reshape(N_BLK * B, N_GRP * B)
    return (left_new, right_new, left_root, right_root, update)
```

```python
import functools

import jax
import jax.numpy as jnp
from jax import lax
from jax.experimental import pallas as pl
from jax.experimental.pallas import tpu as pltpu
from jax.sharding import PartitionSpec as P

B = 512

damping = 0.0001
decay_rate = 0.9
root_order = 4.0
growth = (1.0 + root_order) / root_order

NN = (((1,), (0,)), ((), ()))
NT = (((1,), (1,)), ((), ()))
TN = (((0,), (0,)), ((), ()))


def product(left, right, dims=NN):
    return lax.dot_general(left, right, dims, preferred_element_type=jnp.float32)


def slot_kernel(
    rows_dev,
    steps_ref,
    received_ref,
    stats_left_ref,
    stats_right_ref,
    root_left_ref,
    root_right_ref,
    new_left_ref,
    new_right_ref,
    new_root_left_ref,
    new_root_right_ref,
    pieces_ref,
    grad_ref,
    moving_ref,
    moving_low_ref,
    total_ref,
    mixed_ref,
    side_ref,
    side_low_ref,
):
    owners, rows_all, _ = received_ref.shape
    share = rows_all // rows_dev
    for part in range(share):
        for owner in range(owners):
            start = (part * owners + owner) * rows_dev
            grad_ref[start : start + rows_dev, :] = received_ref[
                owner, part * rows_dev : (part + 1) * rows_dev, :
            ]
    grad = grad_ref[...]
    gram_weight = (1.0 - decay_rate) / B
    new_left_ref[0] = decay_rate * stats_left_ref[0] + gram_weight * product(grad, grad, NT)
    new_right_ref[0] = decay_rate * stats_right_ref[0] + gram_weight * product(grad, grad, TN)
    steps = steps_ref[0]

    @pl.when(steps <= 0)
    def keep():
        new_root_left_ref[...] = root_left_ref[...]
        new_root_right_ref[...] = root_right_ref[...]

    @pl.when(steps > 0)
    def refresh():
        rows = lax.broadcasted_iota(jnp.int32, (B, B), 0)
        columns = lax.broadcasted_iota(jnp.int32, (B, B), 1)
        on_diagonal = rows == columns
        scalings = []
        for side, statistic_ref in enumerate((new_left_ref, new_right_ref)):
            shifted = statistic_ref[0] + jnp.where(on_diagonal, damping, 0.0)
            frobenius = jnp.sqrt(jnp.sum(shifted * shifted, keepdims=True))
            scalings.append(jnp.sqrt(jnp.sqrt((1.0 + root_order) / (2.0 * frobenius))))
            moving = shifted * (0.5 / frobenius)
            moving_ref[side] = moving
            moving_low_ref[side] = moving.astype(jnp.bfloat16)
            total_ref[side] = moving

        def newton(unused, scale):
            for side in range(2):
                low = moving_low_ref[side]
                mixed_ref[side] = (2.0 * moving_ref[side] - product(low, low)).astype(jnp.bfloat16)
            for side in range(2):
                side_ref[side] = product(mixed_ref[side], moving_low_ref[side])
                side_low_ref[side] = side_ref[side].astype(jnp.bfloat16)
            for side in range(2):
                moving = moving_ref[side] - 2.0 * side_ref[side]
                moving = growth**4 * (moving + product(mixed_ref[side], side_low_ref[side]))
                moving_ref[side] = moving
                moving_low_ref[side] = moving.astype(jnp.bfloat16)
            for side in range(2):
                total = total_ref[side]
                total_ref[side] = (
                    total
                    + moving_ref[side]
                    - product(total.astype(jnp.bfloat16), moving_low_ref[side])
                )
            return scale * growth

        scale = lax.fori_loop(1, steps, newton, jnp.float32(growth))
        for side, root_ref in enumerate((new_root_left_ref, new_root_right_ref)):
            root = jnp.where(on_diagonal, 1.0, 0.0) - total_ref[side]
            root_ref[0] = (root * (scalings[side] * scale)).astype(jnp.bfloat16)

    half = product(grad, new_root_right_ref[0]).astype(jnp.bfloat16)
    precon = product(new_root_left_ref[0], half)
    grad_wide = grad.astype(jnp.float32)
    entries = float(B * B)
    grad_mean = jnp.sum(grad_wide * grad_wide, keepdims=True) / entries
    precon_mean = jnp.sum(precon * precon, keepdims=True) / entries
    graft_ratio = jnp.sqrt(grad_mean) / jnp.sqrt(precon_mean + 1e-06)
    update = (precon * graft_ratio).astype(jnp.bfloat16)
    for part in range(share):
        for owner in range(owners):
            start = (part * owners + owner) * rows_dev
            pieces_ref[owner, part * rows_dev : (part + 1) * rows_dev, :] = update[
                start : start + rows_dev, :
            ]


def slot_step(rows_dev, steps, received, stats_left, stats_right, root_left, root_right):
    in_vmem = pl.BlockSpec(memory_space=pltpu.VMEM)
    wide = jax.ShapeDtypeStruct((1, B, B), jnp.float32)
    low = jax.ShapeDtypeStruct((1, B, B), jnp.bfloat16)
    return pl.pallas_call(
        functools.partial(slot_kernel, rows_dev),
        out_shape=(wide, wide, low, low, jax.ShapeDtypeStruct(received.shape, jnp.bfloat16)),
        in_specs=[pl.BlockSpec(memory_space=pltpu.SMEM)] + [in_vmem] * 5,
        out_specs=(in_vmem,) * 5,
        scratch_shapes=[
            pltpu.VMEM((B, B), jnp.bfloat16),
            pltpu.VMEM((2, B, B), jnp.float32),
            pltpu.VMEM((2, B, B), jnp.bfloat16),
            pltpu.VMEM((2, B, B), jnp.float32),
            pltpu.VMEM((2, B, B), jnp.bfloat16),
            pltpu.VMEM((2, B, B), jnp.float32),
            pltpu.VMEM((2, B, B), jnp.bfloat16),
        ],
        compiler_params=pltpu.CompilerParams(vmem_limit_bytes=40 * 1024 * 1024),
        cost_estimate=pl.CostEstimate(flops=20 * 2 * B**3, bytes_accessed=8 * 2**20, transcendentals=0),
        name="slot_step",
    )(steps, received, stats_left, stats_right, root_left, root_right)


def per_device(
    gradient,
    stats_left,
    stats_right,
    root_left,
    root_right,
    slot_block,
    refresh_slots,
    newton_steps,
):
    groups = lax.axis_size("grp")
    owners = lax.axis_size("blk")
    rows_dev = gradient.shape[0]
    group_share = groups // owners
    group_id = lax.axis_index("grp")
    owner_id = lax.axis_index("blk")
    slot_order = lax.dynamic_index_in_dim(slot_block, group_id, 0, keepdims=False)
    positions = jnp.arange(owners, dtype=jnp.int32)
    matches = slot_order[None, :] == positions[:, None]
    inverse = jnp.sum(jnp.where(matches, positions[None, :], 0), axis=1)
    my_slot = group_id * owners + owner_id
    steps_mine = jnp.sum(jnp.where(refresh_slots == my_slot, newton_steps, 0))

    gathered = lax.all_to_all(gradient, "grp", split_axis=1, concat_axis=0, tiled=True)
    by_row = gathered.reshape(owners, group_share * rows_dev, B)
    arranged = by_row.at[slot_order].get(mode="promise_in_bounds")
    received = lax.all_to_all(arranged, "blk", split_axis=0, concat_axis=0, tiled=True)
    left_new, right_new, left_root, right_root, pieces = slot_step(
        rows_dev, steps_mine.reshape(1), received, stats_left, stats_right, root_left, root_right
    )
    returned_rows = lax.all_to_all(pieces, "blk", split_axis=0, concat_axis=0, tiled=True)
    ordered = returned_rows.at[inverse].get(mode="promise_in_bounds")
    ordered = ordered.reshape(groups * rows_dev, B)
    update_rows = lax.all_to_all(ordered, "grp", split_axis=0, concat_axis=1, tiled=True)
    return (left_new, right_new, left_root, right_root, update_rows)


def solution(mesh):
    placed = (
        P(("grp", "blk"), None),
        P(("grp", "blk"), None, None),
        P(("grp", "blk"), None, None),
        P(("grp", "blk"), None, None),
        P(("grp", "blk"), None, None),
        P(),
        P(),
        P(),
    )
    return jax.shard_map(
        per_device,
        mesh=mesh,
        in_specs=placed,
        out_specs=(
            P(("grp", "blk"), None, None),
            P(("grp", "blk"), None, None),
            P(("grp", "blk"), None, None),
            P(("grp", "blk"), None, None),
            P(("grp", "blk"), None),
        ),
        check_vma=False,
    )
```

```python
import functools

import jax
import jax.numpy as jnp
from jax import lax
from jax.experimental import pallas as pl
from jax.experimental.pallas import tpu as pltpu
from jax.sharding import PartitionSpec as P

B = 512

damping = 0.0001
decay_rate = 0.9
root_order = 4.0
growth = (1.0 + root_order) / root_order

NN = (((1,), (0,)), ((), ()))
NT = (((1,), (1,)), ((), ()))
TN = (((0,), (0,)), ((), ()))


def product(left, right, dims=NN):
    return lax.dot_general(left, right, dims, preferred_element_type=jnp.float32)


def block_row(slots_ref, wanted):
    slots = slots_ref[...]
    slot = lax.broadcasted_iota(jnp.int32, slots.shape, 0)
    column = lax.broadcasted_iota(jnp.int32, slots.shape, 1)
    mine = (column == lax.axis_index("grp")) & (slot == wanted)
    return jnp.sum(jnp.where(mine, slots, 0))


def order_kernel(slots_ref, refresh_slots_ref, newton_steps_ref, by_row_ref, steps_ref, *piece_refs):
    owners = by_row_ref.shape[0]
    owner = lax.axis_index("blk")
    refreshed = refresh_slots_ref[...] == lax.axis_index("grp") * owners + owner
    steps = jnp.sum(jnp.where(refreshed, newton_steps_ref[...], 0), axis=1, keepdims=True)
    steps_ref[...] = jnp.broadcast_to(steps, steps_ref.shape)
    for away, piece_ref in zip(distances(owners), piece_refs):
        piece_ref[...] = by_row_ref[block_row(slots_ref, lax.rem(owner + away, owners))]


def restore_kernel(slots_ref, *refs):
    by_row_ref = refs[-1]
    owners = by_row_ref.shape[0]
    owner = lax.axis_index("blk")
    for away, piece_ref in zip(distances(owners), refs[:-1]):
        source = lax.rem(owner + owners - away, owners)
        by_row_ref[block_row(slots_ref, source)] = piece_ref[...]


def distances(owners):
    half = owners // 2
    out = [0, half]
    for step in range(1, half):
        out += [half - step, half + step]
    return out


def exchange(pieces):
    owners = len(pieces)
    return [
        lax.ppermute(piece, "blk", [(i, (i + away) % owners) for i in range(owners)]) if away else piece
        for away, piece in zip(distances(owners), pieces)
    ]


def small_call(kernel, out_shape, *operands):
    in_vmem = pl.BlockSpec(memory_space=pltpu.VMEM)
    return pl.pallas_call(
        kernel,
        out_shape=out_shape,
        in_specs=[in_vmem] * len(operands),
        out_specs=[in_vmem] * len(out_shape),
        compiler_params=pltpu.CompilerParams(vmem_limit_bytes=4 * 1024 * 1024),
        name=kernel.__name__,
    )(*operands)


def slot_kernel(rows_dev, owners, steps_ref, *refs):
    received_refs, refs = refs[:owners], refs[owners:]
    (
        stats_left_ref,
        stats_right_ref,
        root_left_ref,
        root_right_ref,
        new_left_ref,
        new_right_ref,
        new_root_left_ref,
        new_root_right_ref,
    ) = refs[:8]
    piece_refs, refs = refs[8 : 8 + owners], refs[8 + owners :]
    (
        grad_ref,
        moving_ref,
        moving_low_ref,
        total_ref,
        mixed_ref,
        side_ref,
        side_low_ref,
    ) = refs
    owner = lax.axis_index("blk")
    share = B // (owners * rows_dev)
    for away, received_ref in zip(distances(owners), received_refs):
        source = lax.rem(owner + owners - away, owners)
        for part in range(share):
            start = pl.multiple_of((part * owners + source) * rows_dev, rows_dev)
            grad_ref[pl.ds(start, rows_dev), :] = received_ref[
                part * rows_dev : (part + 1) * rows_dev, :
            ]
    grad = grad_ref[...]
    gram_weight = (1.0 - decay_rate) / B
    new_left_ref[0] = decay_rate * stats_left_ref[0] + gram_weight * product(grad, grad, NT)
    new_right_ref[0] = decay_rate * stats_right_ref[0] + gram_weight * product(grad, grad, TN)
    steps = jnp.max(steps_ref[...])

    @pl.when(steps <= 0)
    def keep():
        new_root_left_ref[...] = root_left_ref[...]
        new_root_right_ref[...] = root_right_ref[...]

    @pl.when(steps > 0)
    def refresh():
        rows = lax.broadcasted_iota(jnp.int32, (B, B), 0)
        columns = lax.broadcasted_iota(jnp.int32, (B, B), 1)
        on_diagonal = rows == columns
        scalings = []
        for side, statistic_ref in enumerate((new_left_ref, new_right_ref)):
            shifted = statistic_ref[0] + jnp.where(on_diagonal, damping, 0.0)
            frobenius = jnp.sqrt(jnp.sum(shifted * shifted, keepdims=True))
            scalings.append(jnp.sqrt(jnp.sqrt((1.0 + root_order) / (2.0 * frobenius))))
            moving = shifted * (0.5 / frobenius)
            moving_ref[side] = moving
            moving_low_ref[side] = moving.astype(jnp.bfloat16)
            total_ref[side] = moving

        def newton(unused, scale):
            for side in range(2):
                low = moving_low_ref[side]
                mixed_ref[side] = (2.0 * moving_ref[side] - product(low, low)).astype(jnp.bfloat16)
            for side in range(2):
                side_ref[side] = product(mixed_ref[side], moving_low_ref[side])
                side_low_ref[side] = side_ref[side].astype(jnp.bfloat16)
            for side in range(2):
                moving = moving_ref[side] - 2.0 * side_ref[side]
                moving = growth**4 * (moving + product(mixed_ref[side], side_low_ref[side]))
                moving_ref[side] = moving
                moving_low_ref[side] = moving.astype(jnp.bfloat16)
            for side in range(2):
                total = total_ref[side]
                total_ref[side] = (
                    total
                    + moving_ref[side]
                    - product(total.astype(jnp.bfloat16), moving_low_ref[side])
                )
            return scale * growth

        scale = lax.fori_loop(1, steps, newton, jnp.float32(growth))
        for side, root_ref in enumerate((new_root_left_ref, new_root_right_ref)):
            root = jnp.where(on_diagonal, 1.0, 0.0) - total_ref[side]
            root_ref[0] = (root * (scalings[side] * scale)).astype(jnp.bfloat16)

    half = product(grad, new_root_right_ref[0]).astype(jnp.bfloat16)
    precon = product(new_root_left_ref[0], half)
    grad_wide = grad.astype(jnp.float32)
    entries = float(B * B)
    grad_mean = jnp.sum(grad_wide * grad_wide, keepdims=True) / entries
    precon_mean = jnp.sum(precon * precon, keepdims=True) / entries
    graft_ratio = jnp.sqrt(grad_mean) / jnp.sqrt(precon_mean + 1e-06)
    grad_ref[...] = (precon * graft_ratio).astype(jnp.bfloat16)
    for away, piece_ref in zip(distances(owners), piece_refs):
        target = lax.rem(owner + away, owners)
        for part in range(share):
            start = pl.multiple_of((part * owners + target) * rows_dev, rows_dev)
            piece_ref[part * rows_dev : (part + 1) * rows_dev, :] = grad_ref[pl.ds(start, rows_dev), :]


def slot_step(rows_dev, steps, received, stats_left, stats_right, root_left, root_right):
    in_vmem = pl.BlockSpec(memory_space=pltpu.VMEM)
    wide = jax.ShapeDtypeStruct((1, B, B), jnp.float32)
    low = jax.ShapeDtypeStruct((1, B, B), jnp.bfloat16)
    owners = len(received)
    piece = jax.ShapeDtypeStruct(received[0].shape, received[0].dtype)
    return pl.pallas_call(
        functools.partial(slot_kernel, rows_dev, owners),
        out_shape=[wide, wide, low, low] + [piece] * owners,
        in_specs=[in_vmem] * (5 + owners),
        out_specs=[in_vmem] * (4 + owners),
        scratch_shapes=[
            pltpu.VMEM((B, B), jnp.bfloat16),
            pltpu.VMEM((2, B, B), jnp.float32),
            pltpu.VMEM((2, B, B), jnp.bfloat16),
            pltpu.VMEM((2, B, B), jnp.float32),
            pltpu.VMEM((2, B, B), jnp.bfloat16),
            pltpu.VMEM((2, B, B), jnp.float32),
            pltpu.VMEM((2, B, B), jnp.bfloat16),
        ],
        compiler_params=pltpu.CompilerParams(vmem_limit_bytes=40 * 1024 * 1024),
        cost_estimate=pl.CostEstimate(flops=40 * B**3, bytes_accessed=8 * 2**20, transcendentals=0),
        name="slot_step",
    )(steps, *received, stats_left, stats_right, root_left, root_right)


def per_device(
    gradient,
    stats_left,
    stats_right,
    root_left,
    root_right,
    slot_block,
    refresh_slots,
    newton_steps,
):
    groups = lax.axis_size("grp")
    owners = lax.axis_size("blk")
    rows_dev = gradient.shape[0]
    group_share = groups // owners
    gathered = lax.all_to_all(gradient, "grp", split_axis=1, concat_axis=0, tiled=True)
    by_row = gathered.reshape(owners, group_share * rows_dev, B)
    piece = jax.ShapeDtypeStruct(by_row.shape[1:], by_row.dtype)
    steps, *pieces = small_call(
        order_kernel,
        [jax.ShapeDtypeStruct((1, 128), jnp.int32)] + [piece] * owners,
        slot_block.T,
        refresh_slots[None],
        newton_steps[None],
        by_row,
    )
    left_new, right_new, left_root, right_root, *pieces = slot_step(
        rows_dev, steps, exchange(pieces), stats_left, stats_right, root_left, root_right
    )
    (ordered,) = small_call(
        restore_kernel,
        [jax.ShapeDtypeStruct(by_row.shape, by_row.dtype)],
        slot_block.T,
        *exchange(pieces),
    )
    ordered = ordered.reshape(groups * rows_dev, B)
    update_rows = lax.all_to_all(ordered, "grp", split_axis=0, concat_axis=1, tiled=True)
    return (left_new, right_new, left_root, right_root, update_rows)


def solution(mesh):
    placed = (
        P(("grp", "blk"), None),
        P(("grp", "blk"), None, None),
        P(("grp", "blk"), None, None),
        P(("grp", "blk"), None, None),
        P(("grp", "blk"), None, None),
        P(),
        P(),
        P(),
    )
    return jax.shard_map(
        per_device,
        mesh=mesh,
        in_specs=placed,
        out_specs=(
            P(("grp", "blk"), None, None),
            P(("grp", "blk"), None, None),
            P(("grp", "blk"), None, None),
            P(("grp", "blk"), None, None),
            P(("grp", "blk"), None),
        ),
        check_vma=False,
    )
```

```python
import functools

import jax
import jax.numpy as jnp
from jax import lax
from jax.experimental import pallas as pl
from jax.experimental.pallas import tpu as pltpu
from jax.sharding import PartitionSpec as P

B = 512


damping = 0.0001
decay_rate = 0.9
root_order = 4.0
growth = (1.0 + root_order) / root_order

NN = (((1,), (0,)), ((), ()))
NT = (((1,), (1,)), ((), ()))
TN = (((0,), (0,)), ((), ()))


def product(left, right, dims=NN):
    return lax.dot_general(left, right, dims, preferred_element_type=jnp.float32)


def block_row(slots_ref, wanted):
    slots = slots_ref[...]
    slot = lax.broadcasted_iota(jnp.int32, slots.shape, 0)
    column = lax.broadcasted_iota(jnp.int32, slots.shape, 1)
    mine = (column == lax.axis_index("grp")) & (slot == wanted)
    return jnp.sum(jnp.where(mine, slots, 0))


def order_kernel(
    slots_ref, refresh_slots_ref, newton_steps_ref, by_row_ref, root_left_ref, root_right_ref, steps_ref, *piece_refs
):
    owners = by_row_ref.shape[0]
    owner = lax.axis_index("blk")
    refreshed = refresh_slots_ref[...] == lax.axis_index("grp") * owners + owner
    steps = jnp.sum(jnp.where(refreshed, newton_steps_ref[...], 0), axis=1, keepdims=True)
    steps_ref[...] = jnp.broadcast_to(steps, steps_ref.shape)
    for away, piece_ref in zip(FORWARD, piece_refs):
        piece_ref[...] = by_row_ref[block_row(slots_ref, lax.rem(owner + away, owners))]


def restore_kernel(slots_ref, *refs):
    by_row_ref = refs[-1]
    owners = by_row_ref.shape[0]
    owner = lax.axis_index("blk")
    for away, piece_ref in zip(BACK, refs[:-1]):
        source = lax.rem(owner + owners - away, owners)
        by_row_ref[block_row(slots_ref, source)] = piece_ref[...]


FORWARD = (0, 4, 3, 5, 2, 6, 1, 7)
BACK = (0, 4, 3, 5, 2, 6, 1, 7)


def exchange(pieces, order):
    owners = len(pieces)
    return [
        lax.ppermute(piece, "blk", [(i, (i + away) % owners) for i in range(owners)]) if away else piece
        for away, piece in zip(order, pieces)
    ]


def small_call(kernel, out_shape, *operands):
    in_vmem = pl.BlockSpec(memory_space=pltpu.VMEM)
    return pl.pallas_call(
        kernel,
        out_shape=out_shape,
        in_specs=[in_vmem] * len(operands),
        out_specs=[in_vmem] * len(out_shape),
        compiler_params=pltpu.CompilerParams(vmem_limit_bytes=4 * 1024 * 1024),
        name=kernel.__name__,
    )(*operands)


def slot_kernel(rows_dev, owners, steps_ref, *refs):
    received_refs, refs = refs[:owners], refs[owners:]
    (
        stats_left_ref,
        stats_right_ref,
        root_left_ref,
        root_right_ref,
        new_left_ref,
        new_right_ref,
        new_root_left_ref,
        new_root_right_ref,
    ) = refs[:8]
    piece_refs, refs = refs[8 : 8 + owners], refs[8 + owners :]
    (
        left_ref,
        right_ref,
        left_low_ref,
        right_low_ref,
        copied,
        grad_ref,
        moving_ref,
        moving_low_ref,
        total_ref,
        mixed_ref,
        side_ref,
        side_low_ref,
    ) = refs
    steps = jnp.max(steps_ref[...])
    results = [
        pltpu.make_async_copy(source, target.at[0], copied.at[place])
        for place, (source, target) in enumerate(
            (
                (left_ref, new_left_ref),
                (right_ref, new_right_ref),
                (left_low_ref, new_root_left_ref),
                (right_low_ref, new_root_right_ref),
            )
        )
    ]
    owner = lax.axis_index("blk")
    share = B // (owners * rows_dev)
    for away, received_ref in zip(FORWARD, received_refs):
        source = lax.rem(owner + owners - away, owners)
        for part in range(share):
            start = pl.multiple_of((part * owners + source) * rows_dev, rows_dev)
            grad_ref[pl.ds(start, rows_dev), :] = received_ref[
                part * rows_dev : (part + 1) * rows_dev, :
            ]
    grad = grad_ref[...]
    gram_weight = (1.0 - decay_rate) / B
    left_ref[...] = decay_rate * stats_left_ref[0] + gram_weight * product(grad, grad, NT)
    results[0].start()
    right_ref[...] = decay_rate * stats_right_ref[0] + gram_weight * product(grad, grad, TN)
    results[1].start()

    @pl.when(steps <= 0)
    def keep():
        left_low_ref[...] = root_left_ref[0]
        right_low_ref[...] = root_right_ref[0]

    @pl.when(steps > 0)
    def refresh():
        rows = lax.broadcasted_iota(jnp.int32, (B, B), 0)
        columns = lax.broadcasted_iota(jnp.int32, (B, B), 1)
        on_diagonal = rows == columns
        scalings = []
        for side, statistic_ref in enumerate((left_ref, right_ref)):
            shifted = statistic_ref[...] + jnp.where(on_diagonal, damping, 0.0)
            frobenius = jnp.sqrt(jnp.sum(shifted * shifted, keepdims=True))
            scalings.append(jnp.sqrt(jnp.sqrt((1.0 + root_order) / (2.0 * frobenius))))
            moving = shifted * (0.5 / frobenius)
            moving_ref[side] = moving
            moving_low_ref[side] = moving.astype(jnp.bfloat16)
            total_ref[side] = moving

        def newton(unused, scale):
            for side in range(2):
                low = moving_low_ref[side]
                mixed_ref[side] = (2.0 * moving_ref[side] - product(low, low)).astype(jnp.bfloat16)
            for side in range(2):
                side_ref[side] = product(mixed_ref[side], moving_low_ref[side])
                side_low_ref[side] = side_ref[side].astype(jnp.bfloat16)
            for side in range(2):
                moving = moving_ref[side] - 2.0 * side_ref[side]
                moving = growth**4 * (moving + product(mixed_ref[side], side_low_ref[side]))
                moving_ref[side] = moving
                moving_low_ref[side] = moving.astype(jnp.bfloat16)
            for side in range(2):
                total = total_ref[side]
                total_ref[side] = (
                    total
                    + moving_ref[side]
                    - product(total.astype(jnp.bfloat16), moving_low_ref[side])
                )
            return scale * growth

        scale = lax.fori_loop(1, steps, newton, jnp.float32(growth))
        for side, root_ref in enumerate((left_low_ref, right_low_ref)):
            root = jnp.where(on_diagonal, 1.0, 0.0) - total_ref[side]
            root_ref[...] = (root * (scalings[side] * scale)).astype(jnp.bfloat16)

    results[2].start()
    results[3].start()
    half = product(grad, right_low_ref[...]).astype(jnp.bfloat16)
    precon = product(left_low_ref[...], half)
    grad_wide = grad.astype(jnp.float32)
    entries = float(B * B)
    grad_mean = jnp.sum(grad_wide * grad_wide, keepdims=True) / entries
    precon_mean = jnp.sum(precon * precon, keepdims=True) / entries
    graft_ratio = jnp.sqrt(grad_mean) / jnp.sqrt(precon_mean + 1e-06)
    grad_ref[...] = (precon * graft_ratio).astype(jnp.bfloat16)
    for away, piece_ref in zip(BACK, piece_refs):
        target = lax.rem(owner + away, owners)
        for part in range(share):
            start = pl.multiple_of((part * owners + target) * rows_dev, rows_dev)
            piece_ref[part * rows_dev : (part + 1) * rows_dev, :] = grad_ref[pl.ds(start, rows_dev), :]
    for copy in results:
        copy.wait()


def slot_step(rows_dev, steps, received, stats_left, stats_right, root_left, root_right):
    in_vmem = pl.BlockSpec(memory_space=pltpu.VMEM)
    in_hbm = pl.BlockSpec(memory_space=pltpu.HBM)
    wide = jax.ShapeDtypeStruct((1, B, B), jnp.float32)
    low = jax.ShapeDtypeStruct((1, B, B), jnp.bfloat16)
    owners = len(received)
    piece = jax.ShapeDtypeStruct(received[0].shape, received[0].dtype)
    return pl.pallas_call(
        functools.partial(slot_kernel, rows_dev, owners),
        out_shape=[wide, wide, low, low] + [piece] * owners,
        in_specs=[in_vmem] * (5 + owners),
        out_specs=[in_hbm] * 4 + [in_vmem] * owners,
        scratch_shapes=[
            pltpu.VMEM((B, B), jnp.float32),
            pltpu.VMEM((B, B), jnp.float32),
            pltpu.VMEM((B, B), jnp.bfloat16),
            pltpu.VMEM((B, B), jnp.bfloat16),
            pltpu.SemaphoreType.DMA((4,)),
            pltpu.VMEM((B, B), jnp.bfloat16),
            pltpu.VMEM((2, B, B), jnp.float32),
            pltpu.VMEM((2, B, B), jnp.bfloat16),
            pltpu.VMEM((2, B, B), jnp.float32),
            pltpu.VMEM((2, B, B), jnp.bfloat16),
            pltpu.VMEM((2, B, B), jnp.float32),
            pltpu.VMEM((2, B, B), jnp.bfloat16),
        ],
        compiler_params=pltpu.CompilerParams(vmem_limit_bytes=24 * 1024 * 1024),
        cost_estimate=pl.CostEstimate(flops=40 * B**3, bytes_accessed=8 * 2**20, transcendentals=0),
        name="slot_step",
    )(steps, *received, stats_left, stats_right, root_left, root_right)


def per_device(
    gradient,
    stats_left,
    stats_right,
    root_left,
    root_right,
    slot_block,
    refresh_slots,
    newton_steps,
):
    groups = lax.axis_size("grp")
    owners = lax.axis_size("blk")
    rows_dev = gradient.shape[0]
    group_share = groups // owners
    gathered = lax.all_to_all(gradient, "grp", split_axis=1, concat_axis=0, tiled=True)
    by_row = gathered.reshape(owners, group_share * rows_dev, B)
    piece = jax.ShapeDtypeStruct(by_row.shape[1:], by_row.dtype)
    steps, *pieces = small_call(
        order_kernel,
        [jax.ShapeDtypeStruct((1, 128), jnp.int32)] + [piece] * owners,
        slot_block.T,
        refresh_slots[None],
        newton_steps[None],
        by_row,
        root_left,
        root_right,
    )
    left_new, right_new, left_root, right_root, *pieces = slot_step(
        rows_dev, steps, exchange(pieces, FORWARD), stats_left, stats_right, root_left, root_right
    )
    (ordered,) = small_call(
        restore_kernel,
        [jax.ShapeDtypeStruct(by_row.shape, by_row.dtype)],
        slot_block.T,
        *exchange(pieces, BACK),
    )
    ordered = ordered.reshape(groups * rows_dev, B)
    update_rows = lax.all_to_all(ordered, "grp", split_axis=0, concat_axis=1, tiled=True)
    return (left_new, right_new, left_root, right_root, update_rows)


def solution(mesh):
    placed = (
        P(("grp", "blk"), None),
        P(("grp", "blk"), None, None),
        P(("grp", "blk"), None, None),
        P(("grp", "blk"), None, None),
        P(("grp", "blk"), None, None),
        P(),
        P(),
        P(),
    )
    return jax.shard_map(
        per_device,
        mesh=mesh,
        in_specs=placed,
        out_specs=(
            P(("grp", "blk"), None, None),
            P(("grp", "blk"), None, None),
            P(("grp", "blk"), None, None),
            P(("grp", "blk"), None, None),
            P(("grp", "blk"), None),
        ),
        check_vma=False,
    )
```

```python
import functools

import jax
import jax.numpy as jnp
from jax import lax
from jax.experimental import pallas as pl
from jax.experimental.pallas import tpu as pltpu
from jax.sharding import PartitionSpec as P


B = 512


damping = 0.0001
decay_rate = 0.9
root_order = 4.0
growth = (1.0 + root_order) / root_order

NN = (((1,), (0,)), ((), ()))
NT = (((1,), (1,)), ((), ()))
TN = (((0,), (0,)), ((), ()))


def product(left, right, dims=NN):
    return lax.dot_general(left, right, dims, preferred_element_type=jnp.float32)


def block_row(slots_ref, wanted):
    slots = slots_ref[...]
    slot = lax.broadcasted_iota(jnp.int32, slots.shape, 0)
    column = lax.broadcasted_iota(jnp.int32, slots.shape, 1)
    mine = (column == lax.axis_index("grp")) & (slot == wanted)
    return jnp.sum(jnp.where(mine, slots, 0))


def order_kernel(
    slots_ref, refresh_slots_ref, newton_steps_ref, by_row_ref, root_left_ref, root_right_ref, steps_ref, *message_refs
):
    owners = by_row_ref.shape[0]
    owner = lax.axis_index("blk")
    refreshed = refresh_slots_ref[...] == lax.axis_index("grp") * owners + owner
    steps = jnp.sum(jnp.where(refreshed, newton_steps_ref[...], 0), axis=1, keepdims=True)
    steps_ref[...] = jnp.broadcast_to(steps, steps_ref.shape)
    for meant, message_ref in zip(OUT, message_refs):
        for place, away in enumerate(meant):
            message_ref[place] = by_row_ref[block_row(slots_ref, around(owner, away, owners))]


def restore_kernel(slots_ref, *refs):
    by_row_ref = refs[-1]
    owners = by_row_ref.shape[0]
    owner = lax.axis_index("blk")
    for sent, message_ref in zip(IN, refs[:-1]):
        for place, away in enumerate(sent):
            by_row_ref[block_row(slots_ref, around(owner, -away, owners))] = message_ref[place]


OUT = ((3, 4), (-3,), (2,), (-2,), (1,), (-1,), (0,))
IN = ((3,), (-3,), (2,), (-2,), (1, 4), (-1,), (0,))


def shift(message, places):
    groups, owners = lax.axis_size("grp"), lax.axis_size("blk")
    pairs = [
        (group * owners + i, group * owners + (i + (-places if group % 2 else places)) % owners)
        for group in range(groups)
        for i in range(owners)
    ]
    return lax.ppermute(message, ("grp", "blk"), pairs)


def relay_kernel(far_ref, near_ref, message_ref):
    message_ref[0] = near_ref[0]
    message_ref[1] = far_ref[1]


def exchange(messages):
    up3, down3, up2, down2, up1, down1, held = messages
    up3 = shift(up3, 3)
    down3 = shift(down3, -3)
    up2 = shift(up2, 2)
    down2 = shift(down2, -2)
    (up1,) = small_call(relay_kernel, [jax.ShapeDtypeStruct(up3.shape, up3.dtype)], up3, up1)
    up1 = shift(up1, 1)
    down1 = shift(down1, -1)
    return [up3, down3, up2, down2, up1, down1, held]


def around(owner, places, owners):
    mirrored = lax.rem(lax.axis_index("grp"), 2) == 1
    return lax.rem(owner + jnp.where(mirrored, owners - places, owners + places), owners)


def small_call(kernel, out_shape, *operands):
    in_vmem = pl.BlockSpec(memory_space=pltpu.VMEM)
    return pl.pallas_call(
        kernel,
        out_shape=out_shape,
        in_specs=[in_vmem] * len(operands),
        out_specs=[in_vmem] * len(out_shape),
        compiler_params=pltpu.CompilerParams(vmem_limit_bytes=4 * 1024 * 1024),
    )(*operands)


def slot_kernel(rows_dev, owners, steps_ref, *refs):
    received_refs, refs = refs[: len(IN)], refs[len(IN) :]
    (
        stats_left_ref,
        stats_right_ref,
        root_left_ref,
        root_right_ref,
        new_left_ref,
        new_right_ref,
        new_root_left_ref,
        new_root_right_ref,
    ) = refs[:8]
    message_refs, refs = refs[8 : 8 + len(OUT)], refs[8 + len(OUT) :]
    (
        left_ref,
        right_ref,
        left_low_ref,
        right_low_ref,
        copied,
        grad_ref,
        moving_ref,
        moving_low_ref,
        total_ref,
        mixed_ref,
        side_ref,
        side_low_ref,
    ) = refs
    steps = jnp.max(steps_ref[...])
    results = [
        pltpu.make_async_copy(source, target.at[0], copied.at[place])
        for place, (source, target) in enumerate(
            (
                (left_ref, new_left_ref),
                (right_ref, new_right_ref),
                (left_low_ref, new_root_left_ref),
                (right_low_ref, new_root_right_ref),
            )
        )
    ]
    owner = lax.axis_index("blk")
    share = B // (owners * rows_dev)
    for sent, received_ref in zip(IN, received_refs):
        for place, away in enumerate(sent):
            source = around(owner, -away, owners)
            for part in range(share):
                start = pl.multiple_of((part * owners + source) * rows_dev, rows_dev)
                grad_ref[pl.ds(start, rows_dev), :] = received_ref[
                    place, part * rows_dev : (part + 1) * rows_dev, :
                ]
    grad = grad_ref[...]
    gram_weight = (1.0 - decay_rate) / B
    left_ref[...] = decay_rate * stats_left_ref[0] + gram_weight * product(grad, grad, NT)
    results[0].start()
    right_ref[...] = decay_rate * stats_right_ref[0] + gram_weight * product(grad, grad, TN)
    results[1].start()

    @pl.when(steps <= 0)
    def keep():
        left_low_ref[...] = root_left_ref[0]
        right_low_ref[...] = root_right_ref[0]

    @pl.when(steps > 0)
    def refresh():
        rows = lax.broadcasted_iota(jnp.int32, (B, B), 0)
        columns = lax.broadcasted_iota(jnp.int32, (B, B), 1)
        on_diagonal = rows == columns
        scalings = []
        for side, statistic_ref in enumerate((left_ref, right_ref)):
            shifted = statistic_ref[...] + jnp.where(on_diagonal, damping, 0.0)
            frobenius = jnp.sqrt(jnp.sum(shifted * shifted, keepdims=True))
            scalings.append(jnp.sqrt(jnp.sqrt((1.0 + root_order) / (2.0 * frobenius))))
            moving = shifted * (0.5 / frobenius)
            moving_ref[side] = moving
            moving_low_ref[side] = moving.astype(jnp.bfloat16)
            total_ref[side] = moving

        def newton(unused, scale):
            for side in range(2):
                low = moving_low_ref[side]
                mixed_ref[side] = (2.0 * moving_ref[side] - product(low, low)).astype(jnp.bfloat16)
            for side in range(2):
                side_ref[side] = product(mixed_ref[side], moving_low_ref[side])
                side_low_ref[side] = side_ref[side].astype(jnp.bfloat16)
            for side in range(2):
                moving = moving_ref[side] - 2.0 * side_ref[side]
                moving = growth**4 * (moving + product(mixed_ref[side], side_low_ref[side]))
                moving_ref[side] = moving
                moving_low_ref[side] = moving.astype(jnp.bfloat16)
            for side in range(2):
                total = total_ref[side]
                total_ref[side] = (
                    total
                    + moving_ref[side]
                    - product(total.astype(jnp.bfloat16), moving_low_ref[side])
                )
            return scale * growth

        scale = lax.fori_loop(1, steps, newton, jnp.float32(growth))
        for side, root_ref in enumerate((left_low_ref, right_low_ref)):
            root = jnp.where(on_diagonal, 1.0, 0.0) - total_ref[side]
            root_ref[...] = (root * (scalings[side] * scale)).astype(jnp.bfloat16)

    results[2].start()
    results[3].start()
    half = product(grad, right_low_ref[...]).astype(jnp.bfloat16)
    precon = product(left_low_ref[...], half)
    grad_wide = grad.astype(jnp.float32)
    entries = float(B * B)
    grad_mean = jnp.sum(grad_wide * grad_wide, keepdims=True) / entries
    precon_mean = jnp.sum(precon * precon, keepdims=True) / entries
    graft_ratio = jnp.sqrt(grad_mean) / jnp.sqrt(precon_mean + 1e-06)
    grad_ref[...] = (precon * graft_ratio).astype(jnp.bfloat16)
    for meant, message_ref in zip(OUT, message_refs):
        for place, away in enumerate(meant):
            target = around(owner, away, owners)
            for part in range(share):
                start = pl.multiple_of((part * owners + target) * rows_dev, rows_dev)
                message_ref[place, part * rows_dev : (part + 1) * rows_dev, :] = grad_ref[
                    pl.ds(start, rows_dev), :
                ]
    for copy in results:
        copy.wait()


def messages_of(shape, dtype):
    return [jax.ShapeDtypeStruct((len(meant), *shape), dtype) for meant in OUT]


def slot_step(rows_dev, steps, received, stats_left, stats_right, root_left, root_right):
    in_vmem = pl.BlockSpec(memory_space=pltpu.VMEM)
    in_hbm = pl.BlockSpec(memory_space=pltpu.HBM)
    wide = jax.ShapeDtypeStruct((1, B, B), jnp.float32)
    low = jax.ShapeDtypeStruct((1, B, B), jnp.bfloat16)
    owners = lax.axis_size("blk")
    messages = messages_of(received[0].shape[1:], received[0].dtype)
    return pl.pallas_call(
        functools.partial(slot_kernel, rows_dev, owners),
        out_shape=[wide, wide, low, low] + messages,
        in_specs=[in_vmem] * (5 + len(received)),
        out_specs=[in_hbm] * 4 + [in_vmem] * len(messages),
        scratch_shapes=[
            pltpu.VMEM((B, B), jnp.float32),
            pltpu.VMEM((B, B), jnp.float32),
            pltpu.VMEM((B, B), jnp.bfloat16),
            pltpu.VMEM((B, B), jnp.bfloat16),
            pltpu.SemaphoreType.DMA((4,)),
            pltpu.VMEM((B, B), jnp.bfloat16),
            pltpu.VMEM((2, B, B), jnp.float32),
            pltpu.VMEM((2, B, B), jnp.bfloat16),
            pltpu.VMEM((2, B, B), jnp.float32),
            pltpu.VMEM((2, B, B), jnp.bfloat16),
            pltpu.VMEM((2, B, B), jnp.float32),
            pltpu.VMEM((2, B, B), jnp.bfloat16),
        ],
        compiler_params=pltpu.CompilerParams(vmem_limit_bytes=24 * 1024 * 1024),
        cost_estimate=pl.CostEstimate(flops=40 * B**3, bytes_accessed=8 * 2**20, transcendentals=0),
        name="slot_step",
    )(steps, *received, stats_left, stats_right, root_left, root_right)


def per_device(
    gradient,
    stats_left,
    stats_right,
    root_left,
    root_right,
    slot_block,
    refresh_slots,
    newton_steps,
):
    groups = lax.axis_size("grp")
    owners = lax.axis_size("blk")
    rows_dev = gradient.shape[0]
    group_share = groups // owners
    gathered = lax.all_to_all(gradient, "grp", split_axis=1, concat_axis=0, tiled=True)
    by_row = gathered.reshape(owners, group_share * rows_dev, B)
    steps, *messages = small_call(
        order_kernel,
        [jax.ShapeDtypeStruct((1, 128), jnp.int32)] + messages_of(by_row.shape[1:], by_row.dtype),
        slot_block.T,
        refresh_slots[None],
        newton_steps[None],
        by_row,
        root_left,
        root_right,
    )
    received = exchange(messages)
    left_new, right_new, left_root, right_root, *messages = slot_step(
        rows_dev, steps, received, stats_left, stats_right, root_left, root_right
    )
    returned = exchange(messages)
    (ordered,) = small_call(
        restore_kernel,
        [jax.ShapeDtypeStruct(by_row.shape, by_row.dtype)],
        slot_block.T,
        *returned,
    )
    ordered = ordered.reshape(groups * rows_dev, B)
    update_rows = lax.all_to_all(ordered, "grp", split_axis=0, concat_axis=1, tiled=True)
    return (left_new, right_new, left_root, right_root, update_rows)


def solution(mesh):
    placed = (
        P(("grp", "blk"), None),
        P(("grp", "blk"), None, None),
        P(("grp", "blk"), None, None),
        P(("grp", "blk"), None, None),
        P(("grp", "blk"), None, None),
        P(),
        P(),
        P(),
    )
    return jax.shard_map(
        per_device,
        mesh=mesh,
        in_specs=placed,
        out_specs=(
            P(("grp", "blk"), None, None),
            P(("grp", "blk"), None, None),
            P(("grp", "blk"), None, None),
            P(("grp", "blk"), None, None),
            P(("grp", "blk"), None),
        ),
        check_vma=False,
    )
```
